32 devices in a mesh: gx: 8 (over z, x), gy: 4 (over y, core).
Axes of the slice: x: 2, y: 2, z: 4, core: 2. Of those that a mesh axis runs over, the one named last changes fastest.
Arguments:
- source_tiles: bfloat16 [96, 32, 192, 384], P(('gx', 'gy')), may hold values from -6 to 6
- tile_offsets: int32 [2, 96], P(None, ('gx', 'gy')), may hold values from -128 to 896, as said below
- tile_shifts: int32 [96], P(('gx', 'gy')), may hold values from 0 to 63
- tile_counts: int32 [32], P(('gx', 'gy')), may hold values from 1 to 3, as said below
Outputs:
- merged_slab: float32 [32, 1024, 1024], P(None, 'gx', 'gy')
The draws below stay inside these ranges and needn't reach their ends.
Inputs may be any that keep to these rules, and one draw needn't show every extreme that they name: `tile_offsets`: slot k belongs to the device of joined gx+gy index d = k // 3, that is gx index d // 4 and gy index d % 4. Its x offset lies from that gx index times 128 minus 64 up to that gx index times 128; its y offset from the gy index times 256 minus 128 up to the gy index times 256. So every tile covers its owner's whole block. `tile_counts`: entry d counts the used slots of device d; they are its first slots, the others are ignored. Both 1 and 3 occur in every draw.
All inputs are finite; a program needn't handle non-finite values.
Results may differ from the reference program's by a relative error of at most 0.0003.
Values sent between devices are 32-bit elements; how exact they have to be, the bound alone decides.
A program may use at most 192 MiB of HBM per device.

```python
import jax
import jax.numpy as jnp
from jax import lax

NZ = 32
BX = 128
BY = 256
TX = 192
TY = 384
CAP = 3
RAMP = 32
NSHIFT = 64
RX = 64
RY = 128
NX = 1024
NY = 1024
TILES = 96


def draw_tile_offsets(key, part):
    holders = jnp.arange(TILES, dtype=jnp.int32) // CAP
    rows_gy = NY // BY
    column = holders // rows_gy
    row_place = holders % rows_gy
    key_x, key_y = jax.random.split(jax.random.fold_in(key, 11))
    back_x = jax.random.randint(key_x, (TILES,), 0, TX - BX + 1)
    back_y = jax.random.randint(key_y, (TILES,), 0, TY - BY + 1)
    back_x = back_x.at[0].set(TX - BX).at[TILES - 1].set(0)
    back_y = back_y.at[0].set(TY - BY).at[TILES - 1].set(0)
    return jnp.stack([column * BX - back_x, row_place * BY - back_y]).astype(jnp.int32)


def draw_tile_counts(key, part):
    counts = jax.random.randint(jax.random.fold_in(key, 23), (TILES // CAP,), 1, CAP + 1)
    counts = counts.at[0].set(CAP).at[1].set(1)
    return counts.astype(jnp.int32)


def plant(array, stream_key, smallest, top_value):
    longest = array.shape.index(max(array.shape))
    spots = []
    for shift in (0, 1):
        where = [jax.random.randint(jax.random.fold_in(stream_key, axis), (), 0, length) for axis, length in enumerate(array.shape)]
        where[longest] = (where[longest] + shift) % array.shape[longest]
        spots.append(tuple(where))
    return array.at[spots[0]].set(smallest).at[spots[1]].set(top_value)


def block_scale(rng, extent, shards, least, top_value):
    loudness = 1.0
    for dim, parts in shards:
        draws = jax.random.uniform(jax.random.fold_in(jax.random.fold_in(rng, 6), dim), (parts,), jnp.float32, least / len(shards), top_value / len(shards))
        loudness = loudness * jnp.repeat(jnp.exp(draws), extent[dim] // parts).reshape((-1,) + (1,) * (len(extent) - 1 - dim))
    return loudness


def noise(rng, extent, scale, bound, shards=(), kind=jnp.bfloat16):
    entries = scale * jax.random.normal(rng, extent, jnp.float32)
    if shards:
        entries = entries * block_scale(rng, extent, shards, -0.22, 0.18)
    return jnp.clip(entries, -bound, bound).astype(kind)


def setup_inputs(seed: int = 0) -> dict:
    streams_of = jax.random.split(jax.random.key(seed), 5)
    return {
        "source_tiles": noise(streams_of[0], (TILES, NZ, TX, TY), 1.0, 6.0, ((0, 32),)),
        "tile_offsets": draw_tile_offsets(jax.random.fold_in(streams_of[4], 71), 0),
        "tile_shifts": plant(jax.random.randint(streams_of[2], (TILES,), 0, NSHIFT), jax.random.fold_in(streams_of[2], 1), 0, NSHIFT - 1).astype(jnp.int32),
        "tile_counts": draw_tile_counts(jax.random.fold_in(streams_of[4], 71), 0),
    }


def interpolate(volume, fraction, dimension):
    length = volume.shape[dimension]
    shifted = jnp.concatenate([lax.slice_in_dim(volume, 1, length, axis=dimension), lax.slice_in_dim(volume, length - 1, length, axis=dimension)], axis=dimension)
    return (1.0 - fraction) * volume + fraction * shifted


def resample(source, shift_code):
    depth_part = ((shift_code // 16) % 4).astype(jnp.float32) * 0.25
    column_part = ((shift_code // 4) % 4).astype(jnp.float32) * 0.25
    row_part = (shift_code % 4).astype(jnp.float32) * 0.25
    volume = source.astype(jnp.float32)
    volume = interpolate(volume, depth_part, 0)
    volume = interpolate(volume, column_part, 1)
    return interpolate(volume, row_part, 2)


def blend_ramp(length):
    places = jnp.arange(length, dtype=jnp.float32)
    return jnp.minimum(jnp.minimum(places + 1.0, length - places), float(RAMP))


def reference(source_tiles, tile_offsets, tile_shifts, tile_counts):
    weight_plane = blend_ramp(TX)[:, None] * blend_ramp(TY)[None, :]
    values = jnp.zeros((NZ, NX + 2 * RX, NY + 2 * RY), jnp.float32)
    weights = jnp.zeros((NX + 2 * RX, NY + 2 * RY), jnp.float32)

    def place_tile(accumulated, number):
        values, weights = accumulated
        holder = number // CAP
        active = ((number % CAP) < tile_counts[holder]).astype(jnp.float32)
        source = lax.dynamic_index_in_dim(source_tiles, number, 0, keepdims=False)
        scaled = active * weight_plane
        volume = resample(source, tile_shifts[number]) * scaled[None]
        start_x = (tile_offsets[0, number] + RX).astype(jnp.int32)
        start_y = (tile_offsets[1, number] + RY).astype(jnp.int32)
        anchor = jnp.int32(0)
        window = lax.dynamic_slice(values, (anchor, start_x, start_y), (NZ, TX, TY))
        values = lax.dynamic_update_slice(values, window + volume, (anchor, start_x, start_y))
        weight_window = lax.dynamic_slice(weights, (start_x, start_y), (TX, TY))
        weights = lax.dynamic_update_slice(weights, weight_window + scaled, (start_x, start_y))
        return (values, weights), None

    (values, weights), ignored = lax.scan(place_tile, (values, weights), jnp.arange(TILES, dtype=jnp.int32))
    block_weights = weights[RX:RX + NX, RY:RY + NY]
    return values[:, RX:RX + NX, RY:RY + NY] / jnp.maximum(block_weights, 1.0)[None]
```

```python
import functools

import jax
import jax.numpy as jnp
from jax import lax
from jax.experimental import pallas as pl
from jax.experimental.pallas import tpu as pltpu
from jax.sharding import PartitionSpec as P

BX = 128
BY = 256
RAMP = 32
RX = 64
RY = 128
RING = 4
GROUP = 4
HEAD = 8
FIRST = ((0, 1), (1, 1), (2, 1), (3, 1), (4, 2), (6, 2))
TURNS = 4
FIRST_TURN = ((0, 2), (1, 3), (2, 0), (3, 1), (0, 2), (1, 3))
GROUP_TURN = ((0, 2), (1, 3), (0, 2), (1, 0), (1, 2), (3, 3))
FLIGHT = 8
LAG_NEAR = 1
LAG_FAR = 3
LAG_PLACE = 2
LANES = 128
MESH = pl.DeviceIdType.MESH


def ramp_at(place, length):
    place = place.astype(jnp.float32)
    ramp = jnp.minimum(jnp.minimum(place + 1.0, length - place), float(RAMP))
    return jnp.maximum(ramp, 0.0)


def whole_iota(shape, dimension):
    return lax.broadcasted_iota(jnp.int32, shape, dimension)


def pick(index, options):
    chosen = options[-1]
    for number in range(len(options) - 2, -1, -1):
        chosen = jnp.where(index == number, options[number], chosen)
    return chosen


def kernel(
    grid_x, grid_y, offsets_hbm, shifts_hbm, counts_hbm, tiles_ref, out_ref,
    offsets_ref, shifts_ref, counts_ref,
    planes, strips, arrived, relay, edges, edges_in, middles, middles_in, places,
    across, along, held, parts, scale,
    small_sem, plane_sem, strip_sent, strip_sem, relay_sent, relay_sem,
    edge_sent, edge_sem, middle_sent, middle_sem, place_sent, place_sem,
):
    slots, count, length, rows = tiles_ref.shape
    extent_x, extent_y = across.shape[0], along.shape[2]
    half = extent_y // 2
    groups = count // GROUP
    pairs = grid_x // 2
    column, row = lax.axis_index("gx"), lax.axis_index("gy")
    even = column % 2 == 0
    pair = column // 2
    has_left, has_right = column > 0, column < grid_x - 1
    has_below, has_above = row > 0, row < grid_y - 1
    far_left, far_right = column > 1, column < grid_x - 2
    to_left, to_right = (column - 1, row), (column + 1, row)
    to_below, to_above = (column, row - 1), (column, row + 1)
    to_far_left, to_far_right = (column - 2, row), (column + 2, row)
    odd_row = row % 2 == 1
    near, far = (row + 1) % 2, row % 2
    has_near = (odd_row & has_below) | (jnp.logical_not(odd_row) & has_above)
    has_far = (odd_row & has_above) | (jnp.logical_not(odd_row) & has_below)

    def remote(source, target, sent, done, device):
        return pltpu.make_async_remote_copy(
            src_ref=source, dst_ref=target, send_sem=sent, recv_sem=done,
            device_id=device, device_id_type=MESH,
        )

    def fetch(n):
        slot = n % RING
        return pltpu.make_async_copy(tiles_ref.at[:, n], planes.at[slot], plane_sem.at[slot])

    def edge_below(n):
        return remote(
            edges.at[0, n], edges_in.at[1, n], edge_sent.at[0], edge_sem.at[1, n % FLIGHT], to_below
        )

    def edge_above(n):
        return remote(
            edges.at[1, n], edges_in.at[0, n], edge_sent.at[1], edge_sem.at[0, n % FLIGHT], to_above
        )

    def whole_edges(side, device):
        return remote(
            edges.at[side], edges_in.at[1 - side], edge_sent.at[side], edge_sem.at[1 - side, 0], device
        )

    def middle(side, device):
        return remote(
            middles.at[side], middles_in.at[1 - side], middle_sent.at[side], middle_sem.at[1 - side], device
        )

    def stage_of(start):
        return start // HEAD

    def strip(side, unit, part, device):
        number, start, size, turns = unit
        span = pl.ds(start, size)
        return remote(
            strips.at[side, part, span], arrived.at[1 - side, span, part],
            strip_sent.at[side], strip_sem.at[1 - side, stage_of(start)], device,
        )

    def whole_stage(side, stage):
        span = pl.ds(stage * HEAD, HEAD)
        return remote(
            arrived.at[side, span], arrived.at[side, span],
            strip_sent.at[side], strip_sem.at[side, stage], to_left,
        )

    def whole_strips(side, device):
        return remote(
            strips.at[side], strips.at[side], strip_sent.at[side], strip_sem.at[side, 0], device
        )

    def detour(side, unit, part, device):
        number, start, size, turns = unit
        span = pl.ds(start, size)
        return remote(
            strips.at[side, part, span], relay.at[part, span],
            strip_sent.at[side], relay_sem.at[part, number], device,
        )

    def onward(side, unit, part, device):
        number, start, size, turns = unit
        span = pl.ds(start, size)
        return remote(
            relay.at[part, span], arrived.at[1 - side, span, part],
            relay_sent.at[part, number], strip_sem.at[1 - side, stage_of(start)], device,
        )

    def turn(unit, part):
        lower, upper = unit[3]
        return jnp.where(part == 0, lower, upper)

    def by_relay_left(unit, part):
        return turn(unit, part) * pairs < TURNS * pair

    def by_relay_right(unit, part):
        return turn(unit, part) * pairs < TURNS * (pairs - 1 - pair)

    def send_unit(unit, part):
        turns_left = even & by_relay_left(unit, part)
        turns_right = jnp.logical_not(even) & by_relay_right(unit, part)

        @pl.when(has_left & turns_left)
        def _():
            detour(0, unit, part, to_right).start()

        @pl.when(has_left & jnp.logical_not(turns_left))
        def _():
            strip(0, unit, part, to_left).start()

        @pl.when(has_right & turns_right)
        def _():
            detour(1, unit, part, to_left).start()

        @pl.when(has_right & jnp.logical_not(turns_right))
        def _():
            strip(1, unit, part, to_right).start()

    first_units = [
        (number, start, size, FIRST_TURN[number]) for number, (start, size) in enumerate(FIRST)
    ]

    def group_unit(g):
        kinds = len(GROUP_TURN)
        place = (g - HEAD // GROUP) % kinds
        turns = tuple(pick(place, [GROUP_TURN[i][part] for i in range(kinds)]) for part in (0, 1))
        return len(FIRST) - HEAD // GROUP + g, g * GROUP, GROUP, turns

    def relays_right(unit, part):
        return even & far_right & by_relay_right(unit, part)

    def relays_left(unit, part):
        return jnp.logical_not(even) & far_left & by_relay_left(unit, part)

    def relay_unit(unit):
        for part in (near, far):
            @pl.when(relays_right(unit, part))
            def _():
                detour(1, unit, part, to_left).wait_recv()
                onward(1, unit, part, to_far_right).start()

            @pl.when(relays_left(unit, part))
            def _():
                detour(0, unit, part, to_right).wait_recv()
                onward(0, unit, part, to_far_left).start()

    def relay_done(unit):
        for part in (0, 1):
            @pl.when(relays_right(unit, part))
            def _():
                onward(1, unit, part, to_far_right).wait_send()

            @pl.when(relays_left(unit, part))
            def _():
                onward(0, unit, part, to_far_left).wait_send()

    def place_copy(first, size, target, number, device):
        return remote(
            places.at[pl.ds(first, size)], places.at[pl.ds(target, size)],
            place_sent.at[number], place_sem.at[number], device,
        )

    place_above = place_copy(0, 1, 1, 0, to_above)
    place_below = place_copy(0, 1, 2, 1, to_below)
    place_right = place_copy(0, 3, 3, 2, to_right)
    place_left = place_copy(0, 3, 6, 3, to_left)

    def along_rows(slot, k):
        plane = planes[slot, k]
        low = jnp.dot(plane, along[k, :, :half], preferred_element_type=jnp.float32)
        cut = half - RY
        high = jnp.dot(plane[:, cut:], along[k, cut:, half:], preferred_element_type=jnp.float32)
        return low, high

    small = [
        pltpu.make_async_copy(source, target, small_sem.at[number])
        for number, (source, target) in enumerate(
            ((offsets_hbm, offsets_ref), (shifts_hbm, shifts_ref), (counts_hbm, counts_ref))
        )
    ]
    for copy in small:
        copy.start()
    barrier = pltpu.get_barrier_semaphore()
    peers = (
        (has_left, to_left), (has_right, to_right), (has_below, to_below), (has_above, to_above),
        (far_left, to_far_left), (far_right, to_far_right),
    )
    for there, device in peers:
        @pl.when(there)
        def _():
            pl.semaphore_signal(barrier, inc=1, device_id=device, device_id_type=MESH)
    for n in range(RING):
        fetch(n).start()
    for copy in small:
        copy.wait()

    starts_x = [offsets_ref[0, k] - column * BX for k in range(slots)]
    starts_y = [offsets_ref[1, k] - row * BY for k in range(slots)]
    active = [jnp.where(k < counts_ref[0, 0], 1.0, 0.0) for k in range(slots)]
    shape = places.shape[1:]
    lane, tile = whole_iota(shape, 1), whole_iota(shape, 0)
    record = jnp.zeros(shape, jnp.float32)
    for k in range(slots):
        values = (starts_x[k].astype(jnp.float32), starts_y[k].astype(jnp.float32), active[k])
        for place, value in enumerate(values):
            record = jnp.where((tile == k) & (lane == place), value, record)
    places[0] = record
    for number in range(1, places.shape[0]):
        there = (has_below, has_above, has_left, has_right)[
            number - 1 if number < 3 else number // 3 + 1
        ]

        @pl.when(jnp.logical_not(there))
        def _():
            places[number] = jnp.zeros(shape, jnp.float32)

    for k in range(slots):
        fraction = (shifts_ref[k] % 4).astype(jnp.float32) * 0.25
        target = whole_iota((1, extent_y), 1) - (starts_y[k] + RY)
        ramp = ramp_at(target, rows)
        here = jnp.where(target == rows - 1, ramp, ramp * (1.0 - fraction))
        after = ramp * fraction
        for first, lanes in ((0, slice(0, half)), (half - RY, slice(half, extent_y))):
            source = whole_iota((rows - first, half), 0) + first
            blend = jnp.where(
                source == target[:, lanes], here[:, lanes],
                jnp.where(source == target[:, lanes] + 1, after[:, lanes], 0.0),
            )
            along[k, first:, lanes] = blend.astype(jnp.bfloat16)
    wide = 2 * slots * length
    number = whole_iota((1, wide), 1)
    part = number // length
    source = number - part * length
    part = part // 2
    fraction = pick(
        part, [(shifts_ref[k] // 4 % 4).astype(jnp.float32) * 0.25 for k in range(slots)]
    )
    weight = pick(part, active)
    ramp = ramp_at(source, length) * weight
    here = jnp.where(source == length - 1, ramp, ramp * (1.0 - fraction))
    after = ramp_at(source - 1, length) * weight * fraction
    target = source + pick(part, [start + RX for start in starts_x])
    cell = whole_iota((extent_x, wide), 0)
    blend = jnp.where(cell == target, here, jnp.where(cell == target - 1, after, 0.0))
    across[...] = blend.astype(jnp.bfloat16)

    fetch(0).wait()
    for k in range(slots):
        low, high = along_rows(0, k)
        held[k, :, :half] = low
        held[k, :, half:] = high
    fetch(RING).start()

    def merge(n, part, there):
        @pl.when((n >= 0) & (n < count))
        def _():
            @pl.when(there & (part == 0))
            def _():
                edge_above(n).wait_recv()

            @pl.when(there & (part == 1))
            def _():
                edge_below(n).wait_recv()

            @pl.when(there)
            def _():
                strips[0, part, n] += edges_in[part, n, :RX]
                strips[1, part, n] += edges_in[part, n, RX:]

            for unit in first_units:
                @pl.when(n == unit[1] + unit[2] - 1)
                def _():
                    send_unit(unit, part)

            @pl.when((n >= HEAD) & (n % GROUP == GROUP - 1))
            def _():
                send_unit(group_unit(n // GROUP), part)

    lag_near = jnp.where(has_near, LAG_NEAR, 0)
    lag_far = jnp.where(has_far, LAG_FAR, 0)

    def step(s, carry):
        @pl.when(s < count)
        def _():
            @pl.when(s < count - 1)
            def _():
                fetch(s + 1).wait()

            slot = jnp.minimum(s + 1, count - 1) % RING
            for k in range(slots):
                fraction = (shifts_ref[k] // 16 % 4).astype(jnp.float32) * 0.25
                for number, later in enumerate(along_rows(slot, k)):
                    lanes = slice(number * half, (number + 1) * half)
                    mixed = held[k, :, lanes] * (1.0 - fraction) + later * fraction
                    held[k, :, lanes] = later
                    top = mixed.astype(jnp.bfloat16)
                    rest = (mixed - top.astype(jnp.float32)).astype(jnp.bfloat16)
                    parts[2 * k * length : (2 * k + 1) * length, lanes] = top
                    parts[(2 * k + 1) * length : (2 * k + 2) * length, lanes] = rest

            @pl.when(s + 1 + RING < count)
            def _():
                fetch(s + 1 + RING).start()

            total = jnp.dot(across[...], parts[...], preferred_element_type=jnp.float32)
            left, centre, right = total[:RX], total[RX : RX + BX], total[RX + BX :]
            edges[0, s, :RX] = left[:, :RY]
            edges[0, s, RX:] = right[:, :RY]
            edges[1, s, :RX] = left[:, RY + BY :]
            edges[1, s, RX:] = right[:, RY + BY :]
            for part in (0, 1):
                strips[0, part, s] = left[:, (part + 1) * RY : (part + 2) * RY]
                strips[1, part, s] = right[:, (part + 1) * RY : (part + 2) * RY]

            @pl.when(s == 0)
            def _():
                pl.semaphore_wait(barrier, sum(jnp.where(there, 1, 0) for there, device in peers))

                @pl.when(has_above)
                def _():
                    place_above.start()

                @pl.when(has_below)
                def _():
                    place_below.start()

            @pl.when(has_below)
            def _():
                edge_below(s).start()

            @pl.when(has_above)
            def _():
                edge_above(s).start()

            middles[0, s] = centre[:, :RY]
            middles[1, s] = centre[:, RY + BY :]
            out_ref[s] = centre[:, RY : RY + BY]

        merge(s - lag_near, near, has_near)
        merge(s - lag_far, far, has_far)

        @pl.when(s == LAG_PLACE)
        def _():
            @pl.when(has_below)
            def _():
                place_above.wait_recv()

            @pl.when(has_above)
            def _():
                place_below.wait_recv()

            @pl.when(has_right)
            def _():
                place_right.start()

            @pl.when(has_left)
            def _():
                place_left.start()

        return carry

    lax.fori_loop(0, count + max(LAG_NEAR, LAG_FAR), step, 0)

    @pl.when(has_below)
    def _():
        middle(0, to_below).start()

    @pl.when(has_above)
    def _():
        middle(1, to_above).start()

    for there, copy in ((has_above, place_above), (has_below, place_below)):
        @pl.when(there)
        def _():
            copy.wait_send()

    @pl.when(has_left)
    def _():
        place_right.wait_recv()
        place_left.wait_send()

    @pl.when(has_right)
    def _():
        place_left.wait_recv()
        place_right.wait_send()

    total = jnp.zeros((BX, BY), jnp.float32)
    cell_x = whole_iota((BX, 1), 0).astype(jnp.float32)
    cell_y = whole_iota((1, BY), 1).astype(jnp.float32)
    for number in range(places.shape[0]):
        origin_x = float((0, -BX, BX)[number // 3])
        origin_y = float((0, -BY, BY)[number % 3])
        for k in range(slots):
            start_x = places[number, k : k + 1, 0:1] + origin_x
            start_y = places[number, k : k + 1, 1:2] + origin_y
            weight = places[number, k : k + 1, 2:3]
            total += (ramp_at(cell_x - start_x, length) * weight) * ramp_at(cell_y - start_y, rows)
    scale[...] = 1.0 / jnp.maximum(total, 1.0)

    for unit in first_units:
        relay_unit(unit)

    def relay_group(g, carry):
        relay_unit(group_unit(g))
        return carry

    lax.fori_loop(HEAD // GROUP, groups, relay_group, 0)

    @pl.when(has_below)
    def _():
        whole_edges(0, to_below).wait_send()
        middle(0, to_below).wait_send()
        middle(1, to_above).wait_recv()

    @pl.when(has_above)
    def _():
        whole_edges(1, to_above).wait_send()
        middle(1, to_above).wait_send()
        middle(0, to_below).wait_recv()

    def finish_stage(stage, carry):
        @pl.when(has_left)
        def _():
            whole_stage(0, stage).wait_recv()

        @pl.when(has_right)
        def _():
            whole_stage(1, stage).wait_recv()

        def finish(i, carry):
            n = stage * HEAD + i

            @pl.when(has_below)
            def _():
                out_ref[n, :, :RY] += middles_in[0, n]

            @pl.when(has_above)
            def _():
                out_ref[n, :, RY:] += middles_in[1, n]

            for part in (0, 1):
                lanes = slice(part * RY, (part + 1) * RY)

                @pl.when(has_left)
                def _():
                    out_ref[n, :RX, lanes] += arrived[0, n, part]

                @pl.when(has_right)
                def _():
                    out_ref[n, BX - RX :, lanes] += arrived[1, n, part]

            out_ref[n] = out_ref[n] * scale[...]
            return carry

        lax.fori_loop(0, HEAD, finish, 0)
        return carry

    lax.fori_loop(0, count // HEAD, finish_stage, 0)

    @pl.when(has_left)
    def _():
        whole_strips(0, to_left).wait_send()

    @pl.when(has_right)
    def _():
        whole_strips(1, to_right).wait_send()

    for unit in first_units:
        relay_done(unit)

    def relay_group_done(g, carry):
        relay_done(group_unit(g))
        return carry

    lax.fori_loop(HEAD // GROUP, groups, relay_group_done, 0)


def local(grid_x, grid_y, tiles, tile_offsets, tile_shifts, tile_counts):
    slots, count, length, rows = tiles.shape
    extent_x, extent_y = BX + 2 * RX, BY + 2 * RY
    units = len(FIRST) + (count - HEAD) // GROUP
    vmem = lambda *shape: pltpu.VMEM(shape, jnp.float32)
    sems = lambda *shape: pltpu.SemaphoreType.DMA(shape)
    return pl.pallas_call(
        functools.partial(kernel, grid_x, grid_y),
        in_specs=[
            pl.BlockSpec(memory_space=pltpu.HBM),
            pl.BlockSpec(memory_space=pltpu.HBM),
            pl.BlockSpec(memory_space=pltpu.HBM),
            pl.BlockSpec(memory_space=pltpu.HBM),
        ],
        out_specs=pl.BlockSpec(memory_space=pltpu.VMEM),
        out_shape=pltpu.VMEM((count, BX, BY), jnp.float32),
        scratch_shapes=[
            pltpu.SMEM((2, slots), jnp.int32),
            pltpu.SMEM((slots,), jnp.int32),
            pltpu.SMEM((1, 1), jnp.int32),
            pltpu.VMEM((RING, slots, length, rows), jnp.bfloat16),
            vmem(2, 2, count, RX, RY),
            vmem(2, count, 2, RX, RY),
            vmem(2, count, RX, RY),
            vmem(2, count, 2 * RX, RY),
            vmem(2, count, 2 * RX, RY),
            vmem(2, count, BX, RY),
            vmem(2, count, BX, RY),
            vmem(9, 8 * pl.cdiv(slots, 8), LANES),
            pltpu.VMEM((extent_x, 2 * slots * length), jnp.bfloat16),
            pltpu.VMEM((slots, rows, extent_y), jnp.bfloat16),
            vmem(slots, length, extent_y),
            pltpu.VMEM((2 * slots * length, extent_y), jnp.bfloat16),
            vmem(BX, BY),
            sems(3), sems(RING),
            sems(2), sems(2, count // HEAD), sems(2, units), sems(2, units),
            sems(2), sems(2, FLIGHT),
            sems(2), sems(2),
            sems(4), sems(4),
        ],
        compiler_params=pltpu.CompilerParams(
            collective_id=0, has_side_effects=True, vmem_limit_bytes=52 * 1024 * 1024,
        ),
        name="merged",
    )(tile_offsets, tile_shifts, tile_counts.reshape(1, 1), tiles)


def solution(mesh):
    placed = (
        P(("gx", "gy"), None, None, None),
        P(None, ("gx", "gy")),
        P(("gx", "gy")),
        P(("gx", "gy")),
    )
    return jax.shard_map(
        functools.partial(local, mesh.shape["gx"], mesh.shape["gy"]),
        mesh=mesh, in_specs=placed, out_specs=P(None, "gx", "gy"), check_vma=False,
    )
```

```python
import functools

import jax
import jax.numpy as jnp
from jax import lax
from jax.experimental import pallas as pl
from jax.experimental.pallas import tpu as pltpu
from jax.sharding import PartitionSpec as P

BX = 128
BY = 256
RAMP = 32
RX = 64
RY = 128
RING = 4
STEPS = (1, 2)
LAST = 2
STAGES = 4
TURNS = 4
FLIGHT = 8
LAG_NEAR = 1
LAG_FAR = 3
LAG_PLACE = 2
LANES = 128
MESH = pl.DeviceIdType.MESH


def ramp_at(place, length):
    place = place.astype(jnp.float32)
    ramp = jnp.minimum(jnp.minimum(place + 1.0, length - place), float(RAMP))
    return jnp.maximum(ramp, 0.0)


def whole_iota(shape, dimension):
    return lax.broadcasted_iota(jnp.int32, shape, dimension)


def pick(index, options):
    chosen = options[-1]
    for number in range(len(options) - 2, -1, -1):
        chosen = jnp.where(index == number, options[number], chosen)
    return chosen


def cut(length, steps):
    sizes = []
    for size in steps:
        if size <= length:
            sizes.append(size)
            length -= size
    return sizes + [length] if length else sizes


def units_of(count):
    tail = count // TURNS
    cuts = [
        (size, turns)
        for size in cut((count - tail) // 3, STEPS)
        for turns in ((0, 1), (2, 0), (1, 2))
    ]
    cuts += [(size, (3, 3)) for size in cut(tail, (LAST,) * (tail // LAST))]
    units, start = [], 0
    for size, turns in cuts:
        units.append((len(units), start, size, turns, max(0, len(units) - len(cuts) + STAGES)))
        start += size
    return units


def kernel(
    grid_x, grid_y, offsets_hbm, shifts_hbm, counts_hbm, tiles_ref, out_ref,
    offsets_ref, shifts_ref, counts_ref,
    planes, strips, arrived, relay, edges, edges_in, middles, middles_in, places,
    across, along, held, parts, scale,
    small_sem, plane_sem, strip_sent, strip_sem, relay_sent, relay_sem,
    edge_sent, edge_sem, middle_sent, middle_sem, place_sent, place_sem,
):
    slots, count, length, rows = tiles_ref.shape
    extent_x, extent_y = across.shape[0], along.shape[2]
    half = extent_y // 2
    units = units_of(count)
    pairs = grid_x // 2
    column, row = lax.axis_index("gx"), lax.axis_index("gy")
    even = column % 2 == 0
    pair = column // 2
    has_left, has_right = column > 0, column < grid_x - 1
    has_below, has_above = row > 0, row < grid_y - 1
    far_left, far_right = column > 1, column < grid_x - 2
    to_left, to_right = (column - 1, row), (column + 1, row)
    to_below, to_above = (column, row - 1), (column, row + 1)
    to_far_left, to_far_right = (column - 2, row), (column + 2, row)
    odd_row = row % 2 == 1
    near, far = (row + 1) % 2, row % 2
    has_near = (odd_row & has_below) | (jnp.logical_not(odd_row) & has_above)
    has_far = (odd_row & has_above) | (jnp.logical_not(odd_row) & has_below)

    def remote(source, target, sent, done, device):
        return pltpu.make_async_remote_copy(
            src_ref=source, dst_ref=target, send_sem=sent, recv_sem=done,
            device_id=device, device_id_type=MESH,
        )

    def fetch(n):
        slot = n % RING
        return pltpu.make_async_copy(tiles_ref.at[:, n], planes.at[:, slot], plane_sem.at[slot])

    def edge_below(n):
        return remote(
            edges.at[0, n], edges_in.at[1, n], edge_sent.at[0], edge_sem.at[1, n % FLIGHT], to_below
        )

    def edge_above(n):
        return remote(
            edges.at[1, n], edges_in.at[0, n], edge_sent.at[1], edge_sem.at[0, n % FLIGHT], to_above
        )

    def whole_edges(side, device):
        return remote(
            edges.at[side], edges_in.at[1 - side], edge_sent.at[side], edge_sem.at[1 - side, 0], device
        )

    def middle(side, device):
        return remote(
            middles.at[side], middles_in.at[1 - side], middle_sent.at[side], middle_sem.at[1 - side], device
        )

    def strip(side, unit, part, device):
        number, start, size, turns, stage = unit
        span = pl.ds(start, size)
        return remote(
            strips.at[side, part, span], arrived.at[1 - side, span, part],
            strip_sent.at[side], strip_sem.at[1 - side, stage], device,
        )

    def whole_stage(side, stage, first, last):
        span = pl.ds(first, last - first)
        return remote(
            arrived.at[side, span], arrived.at[side, span],
            strip_sent.at[side], strip_sem.at[side, stage], to_left,
        )

    def whole_strips(side, device):
        return remote(
            strips.at[side], strips.at[side], strip_sent.at[side], strip_sem.at[side, 0], device
        )

    def detour(side, unit, part, device):
        number, start, size, turns, stage = unit
        span = pl.ds(start, size)
        return remote(
            strips.at[side, part, span], relay.at[part, span],
            strip_sent.at[side], relay_sem.at[part, number], device,
        )

    def onward(side, unit, part, device):
        number, start, size, turns, stage = unit
        span = pl.ds(start, size)
        return remote(
            relay.at[part, span], arrived.at[1 - side, span, part],
            relay_sent.at[turn(unit, part)], strip_sem.at[1 - side, stage], device,
        )

    def turn(unit, part):
        lower, upper = unit[3]
        return jnp.where(part == 0, lower, upper)

    def by_relay_left(unit, part):
        return turn(unit, part) * pairs < TURNS * pair

    def by_relay_right(unit, part):
        return turn(unit, part) * pairs < TURNS * (pairs - 1 - pair)

    def send_unit(unit, part):
        turns_left = even & by_relay_left(unit, part)
        turns_right = jnp.logical_not(even) & by_relay_right(unit, part)

        @pl.when(has_left & turns_left)
        def _():
            detour(0, unit, part, to_right).start()

        @pl.when(has_left & jnp.logical_not(turns_left))
        def _():
            strip(0, unit, part, to_left).start()

        @pl.when(has_right & turns_right)
        def _():
            detour(1, unit, part, to_left).start()

        @pl.when(has_right & jnp.logical_not(turns_right))
        def _():
            strip(1, unit, part, to_right).start()

    def relays_right(unit, part):
        return even & far_right & by_relay_right(unit, part)

    def relays_left(unit, part):
        return jnp.logical_not(even) & far_left & by_relay_left(unit, part)

    def relay_unit(unit):
        for part in (near, far):
            @pl.when(relays_right(unit, part))
            def _():
                detour(1, unit, part, to_left).wait_recv()
                onward(1, unit, part, to_far_right).start()

            @pl.when(relays_left(unit, part))
            def _():
                detour(0, unit, part, to_right).wait_recv()
                onward(0, unit, part, to_far_left).start()

    def relayed(kind):
        span = pl.ds(0, 2 * count // TURNS)
        return remote(
            relay.at[0, span], relay.at[0, span], relay_sent.at[kind], relay_sem.at[0, 0], to_left
        )

    def place_copy(first, size, target, number, device):
        return remote(
            places.at[pl.ds(first, size)], places.at[pl.ds(target, size)],
            place_sent.at[number], place_sem.at[number], device,
        )

    place_above = place_copy(0, 1, 1, 0, to_above)
    place_below = place_copy(0, 1, 2, 1, to_below)
    place_right = place_copy(0, 3, 3, 2, to_right)
    place_left = place_copy(0, 3, 6, 3, to_left)

    def along_rows(plane, k):
        low = jnp.dot(plane, along[k, :, :half], preferred_element_type=jnp.float32)
        cut = half - RY
        high = jnp.dot(plane[:, cut:], along[k, cut:, half:], preferred_element_type=jnp.float32)
        return low, high

    def mix(now, later, k, number):
        lanes = slice(number * half, (number + 1) * half)
        fraction = (shifts_ref[k] // 16 % 4).astype(jnp.float32) * 0.25
        mixed = now * (1.0 - fraction) + later * fraction
        held[k, :, lanes] = later
        top = mixed.astype(jnp.bfloat16)
        rest = (mixed - top.astype(jnp.float32)).astype(jnp.bfloat16)
        parts[2 * k * length : (2 * k + 1) * length, lanes] = top
        parts[(2 * k + 1) * length : (2 * k + 2) * length, lanes] = rest

    small = [
        pltpu.make_async_copy(source, target, small_sem.at[number])
        for number, (source, target) in enumerate(
            ((offsets_hbm, offsets_ref), (shifts_hbm, shifts_ref), (counts_hbm, counts_ref))
        )
    ]
    for copy in small:
        copy.start()
    for n in range(2):
        fetch(n).start()
    barrier = pltpu.get_barrier_semaphore()
    peers = (
        (has_left, to_left), (has_right, to_right), (has_below, to_below), (has_above, to_above),
        (far_left, to_far_left), (far_right, to_far_right),
    )
    for there, device in peers:
        @pl.when(there)
        def _():
            pl.semaphore_signal(barrier, inc=1, device_id=device, device_id_type=MESH)
    for copy in small:
        copy.wait()
    for n in range(2, RING):
        fetch(n).start()

    starts_x = [offsets_ref[0, k] - column * BX for k in range(slots)]
    starts_y = [offsets_ref[1, k] - row * BY for k in range(slots)]
    active = [jnp.where(k < counts_ref[0, 0], 1.0, 0.0) for k in range(slots)]
    shape = places.shape[1:]
    lane, tile = whole_iota(shape, 1), whole_iota(shape, 0)
    record = jnp.zeros(shape, jnp.float32)
    for k in range(slots):
        values = (starts_x[k].astype(jnp.float32), starts_y[k].astype(jnp.float32), active[k])
        for place, value in enumerate(values):
            record = jnp.where((tile == k) & (lane == place), value, record)
    places[0] = record
    for number in range(1, places.shape[0]):
        there = (has_below, has_above, has_left, has_right)[
            number - 1 if number < 3 else number // 3 + 1
        ]

        @pl.when(jnp.logical_not(there))
        def _():
            places[number] = jnp.zeros(shape, jnp.float32)

    for k in range(slots):
        fraction = (shifts_ref[k] % 4).astype(jnp.float32) * 0.25
        target = whole_iota((1, extent_y), 1) - (starts_y[k] + RY)
        ramp = ramp_at(target, rows)
        here = jnp.where(target == rows - 1, ramp, ramp * (1.0 - fraction))
        after = ramp * fraction
        for first, lanes in ((0, slice(0, half)), (half - RY, slice(half, extent_y))):
            source = whole_iota((rows - first, half), 0) + first
            blend = jnp.where(
                source == target[:, lanes], here[:, lanes],
                jnp.where(source == target[:, lanes] + 1, after[:, lanes], 0.0),
            )
            along[k, first:, lanes] = blend.astype(jnp.bfloat16)
    fetch(0).wait()
    fetch(1).wait()
    for k in range(slots):
        both = planes[k, :2].reshape(2 * length, rows)
        for number, rising in enumerate(along_rows(both, k)):
            mix(rising[:length], rising[length:], k, number)
    fetch(RING).start()
    wide = 2 * slots * length
    number = whole_iota((1, wide), 1)
    part = number // length
    source = number - part * length
    part = part // 2
    fraction = pick(
        part, [(shifts_ref[k] // 4 % 4).astype(jnp.float32) * 0.25 for k in range(slots)]
    )
    weight = pick(part, active)
    ramp = ramp_at(source, length) * weight
    here = jnp.where(source == length - 1, ramp, ramp * (1.0 - fraction))
    after = ramp_at(source - 1, length) * weight * fraction
    target = source + pick(part, [start + RX for start in starts_x])
    cell = whole_iota((extent_x, wide), 0)
    blend = jnp.where(cell == target, here, jnp.where(cell == target - 1, after, 0.0))
    across[...] = blend.astype(jnp.bfloat16)

    def merge(n, part, there):
        @pl.when((n >= 0) & (n < count))
        def _():
            @pl.when(there & (part == 0))
            def _():
                edge_above(n).wait_recv()

            @pl.when(there & (part == 1))
            def _():
                edge_below(n).wait_recv()

            @pl.when(there)
            def _():
                strips[0, part, n] += edges_in[part, n, :RX]
                strips[1, part, n] += edges_in[part, n, RX:]

            for unit in units:
                @pl.when(n == unit[1] + unit[2] - 1)
                def _():
                    send_unit(unit, part)

    lag_near = jnp.where(has_near, LAG_NEAR, 0)
    lag_far = jnp.where(has_far, LAG_FAR, 0)

    def outer(s, left, right):
        edges[0, s, :RX] = left[:, :RY]
        edges[0, s, RX:] = right[:, :RY]
        edges[1, s, :RX] = left[:, RY + BY :]
        edges[1, s, RX:] = right[:, RY + BY :]
        for part in (0, 1):
            strips[0, part, s] = left[:, (part + 1) * RY : (part + 2) * RY]
            strips[1, part, s] = right[:, (part + 1) * RY : (part + 2) * RY]

    def send_edges(s):
        @pl.when(has_below)
        def _():
            edge_below(s).start()

        @pl.when(has_above)
        def _():
            edge_above(s).start()

    def inner(s, centre):
        middles[0, s] = centre[:, :RY]
        middles[1, s] = centre[:, RY + BY :]
        out_ref[s] = centre[:, RY : RY + BY]

    def merges(s):
        merge(s - lag_near, near, has_near)
        merge(s - lag_far, far, has_far)

    def step(s, carry):
        @pl.when(s < count)
        def _():
            @pl.when(s < count - 1)
            def _():
                fetch(s + 1).wait()

            slot = jnp.minimum(s + 1, count - 1) % RING
            for k in range(slots):
                for number, later in enumerate(along_rows(planes[k, slot], k)):
                    mix(held[k, :, number * half : (number + 1) * half], later, k, number)

            @pl.when(s + 1 + RING < count)
            def _():
                fetch(s + 1 + RING).start()

            total = jnp.dot(across[...], parts[...], preferred_element_type=jnp.float32)
            outer(s, total[:RX], total[RX + BX :])
            send_edges(s)
            inner(s, total[RX : RX + BX])

        merges(s)

        @pl.when(s == LAG_PLACE)
        def _():
            @pl.when(has_below)
            def _():
                place_above.wait_recv()

            @pl.when(has_above)
            def _():
                place_below.wait_recv()

            @pl.when(has_right)
            def _():
                place_right.start()

            @pl.when(has_left)
            def _():
                place_left.start()

        return carry

    total = jnp.dot(across[...], parts[...], preferred_element_type=jnp.float32)
    outer(0, total[:RX], total[RX + BX :])
    inner(0, total[RX : RX + BX])
    pl.semaphore_wait(barrier, sum(jnp.where(there, 1, 0) for there, device in peers))
    send_edges(0)
    merges(0)

    @pl.when(has_above)
    def _():
        place_above.start()

    @pl.when(has_below)
    def _():
        place_below.start()

    fetch(1 + RING).start()
    lax.fori_loop(1, count + max(LAG_NEAR, LAG_FAR), step, 0)

    for side, there in ((0, has_below), (1, has_above)):
        @pl.when(jnp.logical_not(there))
        def _():
            def clear(n, carry):
                middles_in[side, n] = jnp.zeros(middles_in.shape[2:], jnp.float32)
                return carry

            lax.fori_loop(0, count, clear, 0)

    for side, there in ((0, has_left), (1, has_right)):
        @pl.when(jnp.logical_not(there))
        def _():
            def clear(n, carry):
                arrived[side, n] = jnp.zeros(arrived.shape[2:], jnp.float32)
                return carry

            lax.fori_loop(0, count, clear, 0)

    @pl.when(has_below)
    def _():
        middle(0, to_below).start()

    @pl.when(has_above)
    def _():
        middle(1, to_above).start()

    for there, copy in ((has_above, place_above), (has_below, place_below)):
        @pl.when(there)
        def _():
            copy.wait_send()

    @pl.when(has_left)
    def _():
        place_right.wait_recv()
        place_left.wait_send()

    @pl.when(has_right)
    def _():
        place_left.wait_recv()
        place_right.wait_send()

    total = jnp.zeros((BX, BY), jnp.float32)
    cell_x = whole_iota((BX, 1), 0).astype(jnp.float32)
    cell_y = whole_iota((1, BY), 1).astype(jnp.float32)
    for number in range(places.shape[0]):
        origin_x = float((0, -BX, BX)[number // 3])
        origin_y = float((0, -BY, BY)[number % 3])
        for k in range(slots):
            start_x = places[number, k : k + 1, 0:1] + origin_x
            start_y = places[number, k : k + 1, 1:2] + origin_y
            weight = places[number, k : k + 1, 2:3]
            total += (ramp_at(cell_x - start_x, length) * weight) * ramp_at(cell_y - start_y, rows)
    scale[...] = 1.0 / jnp.maximum(total, 1.0)

    for unit in units:
        relay_unit(unit)

    @pl.when(has_below)
    def _():
        whole_edges(0, to_below).wait_send()
        middle(0, to_below).wait_send()
        middle(1, to_above).wait_recv()

    @pl.when(has_above)
    def _():
        whole_edges(1, to_above).wait_send()
        middle(1, to_above).wait_send()
        middle(0, to_below).wait_recv()

    def finish(n, carry):
        for part in (0, 1):
            lanes = slice(part * RY, (part + 1) * RY)
            for side in (0, 1):
                cells = slice(side * RX, (side + 1) * RX)
                total = out_ref[n, cells, lanes] + middles_in[part, n, cells]
                total += arrived[side, n, part]
                out_ref[n, cells, lanes] = total * scale[cells, lanes]
        return carry

    for stage in range(STAGES):
        inside = [unit for unit in units if unit[4] == stage]
        first, last = inside[0][1], inside[-1][1] + inside[-1][2]

        @pl.when(has_left)
        def _():
            whole_stage(0, stage, first, last).wait_recv()

        @pl.when(has_right)
        def _():
            whole_stage(1, stage, first, last).wait_recv()

        lax.fori_loop(first, last, finish, 0)

    @pl.when(has_left)
    def _():
        whole_strips(0, to_left).wait_send()

    @pl.when(has_right)
    def _():
        whole_strips(1, to_right).wait_send()

    for kind in range(TURNS):
        right = even & far_right & (kind * pairs < TURNS * (pairs - 1 - pair))
        left = jnp.logical_not(even) & far_left & (kind * pairs < TURNS * pair)

        @pl.when(right | left)
        def _():
            relayed(kind).wait_send()


def local(grid_x, grid_y, tiles, tile_offsets, tile_shifts, tile_counts):
    slots, count, length, rows = tiles.shape
    extent_x, extent_y = BX + 2 * RX, BY + 2 * RY
    units = len(units_of(count))
    vmem = lambda *shape: pltpu.VMEM(shape, jnp.float32)
    sems = lambda *shape: pltpu.SemaphoreType.DMA(shape)
    return pl.pallas_call(
        functools.partial(kernel, grid_x, grid_y),
        in_specs=[
            pl.BlockSpec(memory_space=pltpu.HBM),
            pl.BlockSpec(memory_space=pltpu.HBM),
            pl.BlockSpec(memory_space=pltpu.HBM),
            pl.BlockSpec(memory_space=pltpu.HBM),
        ],
        out_specs=pl.BlockSpec(memory_space=pltpu.VMEM),
        out_shape=pltpu.VMEM((count, BX, BY), jnp.float32),
        scratch_shapes=[
            pltpu.SMEM((2, slots), jnp.int32),
            pltpu.SMEM((slots,), jnp.int32),
            pltpu.SMEM((1, 1), jnp.int32),
            pltpu.VMEM((slots, RING, length, rows), jnp.bfloat16),
            vmem(2, 2, count, RX, RY),
            vmem(2, count, 2, RX, RY),
            vmem(2, count, RX, RY),
            vmem(2, count, 2 * RX, RY),
            vmem(2, count, 2 * RX, RY),
            vmem(2, count, BX, RY),
            vmem(2, count, BX, RY),
            vmem(9, 8 * pl.cdiv(slots, 8), LANES),
            pltpu.VMEM((extent_x, 2 * slots * length), jnp.bfloat16),
            pltpu.VMEM((slots, rows, extent_y), jnp.bfloat16),
            vmem(slots, length, extent_y),
            pltpu.VMEM((2 * slots * length, extent_y), jnp.bfloat16),
            vmem(BX, BY),
            sems(3), sems(RING),
            sems(2), sems(2, STAGES), sems(TURNS), sems(2, units),
            sems(2), sems(2, FLIGHT),
            sems(2), sems(2),
            sems(4), sems(4),
        ],
        compiler_params=pltpu.CompilerParams(
            collective_id=0, has_side_effects=True, vmem_limit_bytes=52 * 1024 * 1024,
        ),
        name="merged",
    )(tile_offsets, tile_shifts, tile_counts.reshape(1, 1), tiles)


def solution(mesh):
    placed = (
        P(("gx", "gy"), None, None, None),
        P(None, ("gx", "gy")),
        P(("gx", "gy")),
        P(("gx", "gy")),
    )
    return jax.shard_map(
        functools.partial(local, mesh.shape["gx"], mesh.shape["gy"]),
        mesh=mesh, in_specs=placed, out_specs=P(None, "gx", "gy"), check_vma=False,
    )
```

```python
import functools

import jax
import jax.numpy as jnp
from jax import lax
from jax.experimental import pallas as pl
from jax.experimental.pallas import tpu as pltpu
from jax.sharding import PartitionSpec as P

BX = 128
BY = 256
RAMP = 32
RX = 64
RY = 128
RING = 4
STEPS = (1, 2)
LAST = 2
STAGES = 3
TURNS = 4
FLIGHT = 8
LAG_NEAR = 1
LAG_FAR = 3
LAG_PLACE = 2
LANES = 128
MESH = pl.DeviceIdType.MESH


def ramp_at(place, length):
    place = place.astype(jnp.float32)
    ramp = jnp.minimum(jnp.minimum(place + 1.0, length - place), float(RAMP))
    return jnp.maximum(ramp, 0.0)


def whole_iota(shape, dimension):
    return lax.broadcasted_iota(jnp.int32, shape, dimension)


def pick(index, options):
    chosen = options[-1]
    for number in range(len(options) - 2, -1, -1):
        chosen = jnp.where(index == number, options[number], chosen)
    return chosen


def cut(length, steps):
    sizes = []
    for size in steps:
        if size <= length:
            sizes.append(size)
            length -= size
    return sizes + [length] if length else sizes


def units_of(count):
    tail = count // TURNS
    cuts = [
        (size, turns)
        for size in cut((count - tail) // 3, STEPS)
        for turns in ((0, 1), (2, 0), (1, 2))
    ]
    cuts += [(size, (3, 3)) for size in cut(tail, (LAST,) * (tail // LAST))]
    units, start = [], 0
    for size, turns in cuts:
        units.append((len(units), start, size, turns, max(0, len(units) - len(cuts) + STAGES)))
        start += size
    return units


def kernel(
    grid_x, grid_y, offsets_hbm, shifts_hbm, counts_hbm, tiles_ref, out_ref,
    offsets_ref, shifts_ref, counts_ref,
    planes, strips, arrived, relay, edges, edges_in, middles, middles_in, places,
    across, along, brims, held, parts, scale,
    small_sem, plane_sem, strip_sent, strip_sem, relay_sent, relay_sem,
    edge_sent, edge_sem, middle_sent, middle_sem, place_sent, place_sem,
):
    slots, count, length, rows = tiles_ref.shape
    extent_x, extent_y = across.shape[0], along.shape[2]
    half = extent_y // 2
    units = units_of(count)
    turning = [unit for unit in units if min(unit[3]) < TURNS - 1]
    pairs = grid_x // 2
    column, row = lax.axis_index("gx"), lax.axis_index("gy")
    even = column % 2 == 0
    pair = column // 2
    has_left, has_right = column > 0, column < grid_x - 1
    has_below, has_above = row > 0, row < grid_y - 1
    far_left, far_right = column > 1, column < grid_x - 2
    to_left, to_right = (column - 1, row), (column + 1, row)
    to_below, to_above = (column, row - 1), (column, row + 1)
    to_far_left, to_far_right = (column - 2, row), (column + 2, row)
    odd_row = row % 2 == 1
    near, far = (row + 1) % 2, row % 2
    has_near = (odd_row & has_below) | (jnp.logical_not(odd_row) & has_above)
    has_far = (odd_row & has_above) | (jnp.logical_not(odd_row) & has_below)

    def remote(source, target, sent, done, device):
        return pltpu.make_async_remote_copy(
            src_ref=source, dst_ref=target, send_sem=sent, recv_sem=done,
            device_id=device, device_id_type=MESH,
        )

    def fetch(n):
        slot = n % RING
        return pltpu.make_async_copy(tiles_ref.at[:, n], planes.at[:, slot], plane_sem.at[slot])

    def edge_below(n):
        return remote(
            edges.at[0, n], edges_in.at[1, n], edge_sent.at[0], edge_sem.at[1, n % FLIGHT], to_below
        )

    def edge_above(n):
        return remote(
            edges.at[1, n], edges_in.at[0, n], edge_sent.at[1], edge_sem.at[0, n % FLIGHT], to_above
        )

    def whole_edges(side, device):
        return remote(
            edges.at[side], edges_in.at[1 - side], edge_sent.at[side], edge_sem.at[1 - side, 0], device
        )

    def middle(side, device):
        return remote(
            middles.at[side], middles_in.at[1 - side], middle_sent.at[side], middle_sem.at[1 - side], device
        )

    def strip(side, unit, part, device):
        number, start, size, turns, stage = unit
        span = pl.ds(start, size)
        return remote(
            strips.at[side, part, span], arrived.at[1 - side, span, part],
            strip_sent.at[side], strip_sem.at[1 - side, stage], device,
        )

    def whole_stage(side, stage, first, last):
        span = pl.ds(first, last - first)
        return remote(
            arrived.at[side, span], arrived.at[side, span],
            strip_sent.at[side], strip_sem.at[side, stage], to_left,
        )

    def whole_strips(side, device):
        return remote(
            strips.at[side], strips.at[side], strip_sent.at[side], strip_sem.at[side, 0], device
        )

    def detour(side, unit, part, device):
        number, start, size, turns, stage = unit
        span = pl.ds(start, size)
        return remote(
            strips.at[side, part, span], relay.at[part, span],
            strip_sent.at[side], relay_sem.at[part, number], device,
        )

    def onward(side, unit, part, device):
        number, start, size, turns, stage = unit
        span = pl.ds(start, size)
        return remote(
            relay.at[part, span], arrived.at[1 - side, span, part],
            relay_sent.at[turn(unit, part)], strip_sem.at[1 - side, stage], device,
        )

    def turn(unit, part):
        lower, upper = unit[3]
        return jnp.where(part == 0, lower, upper)

    def by_relay_left(unit, part):
        kind = turn(unit, part)
        return (kind < TURNS - 1) & (kind * pairs < TURNS * pair)

    def by_relay_right(unit, part):
        kind = turn(unit, part)
        return (kind < TURNS - 1) & (kind * pairs < TURNS * (pairs - 1 - pair))

    def send_unit(unit, part):
        if min(unit[3]) == TURNS - 1:
            @pl.when(has_left)
            def _():
                strip(0, unit, part, to_left).start()

            @pl.when(has_right)
            def _():
                strip(1, unit, part, to_right).start()

            return

        turns_left = even & by_relay_left(unit, part)
        turns_right = jnp.logical_not(even) & by_relay_right(unit, part)

        @pl.when(has_left & turns_left)
        def _():
            detour(0, unit, part, to_right).start()

        @pl.when(has_left & jnp.logical_not(turns_left))
        def _():
            strip(0, unit, part, to_left).start()

        @pl.when(has_right & turns_right)
        def _():
            detour(1, unit, part, to_left).start()

        @pl.when(has_right & jnp.logical_not(turns_right))
        def _():
            strip(1, unit, part, to_right).start()

    def relays_right(unit, part):
        return even & far_right & by_relay_right(unit, part)

    def relays_left(unit, part):
        return jnp.logical_not(even) & far_left & by_relay_left(unit, part)

    def relay_unit(unit):
        for part in (near, far):
            @pl.when(relays_right(unit, part))
            def _():
                detour(1, unit, part, to_left).wait_recv()
                onward(1, unit, part, to_far_right).start()

            @pl.when(relays_left(unit, part))
            def _():
                detour(0, unit, part, to_right).wait_recv()
                onward(0, unit, part, to_far_left).start()

    def relayed(kind):
        span = pl.ds(0, 2 * count // TURNS)
        return remote(
            relay.at[0, span], relay.at[0, span], relay_sent.at[kind], relay_sem.at[0, 0], to_left
        )

    def place_copy(first, size, target, number, device):
        return remote(
            places.at[pl.ds(first, size)], places.at[pl.ds(target, size)],
            place_sent.at[number], place_sem.at[number], device,
        )

    place_above = place_copy(0, 1, 1, 0, to_above)
    place_below = place_copy(0, 1, 2, 1, to_below)
    place_right = place_copy(0, 3, 3, 2, to_right)
    place_left = place_copy(0, 3, 6, 3, to_left)

    def along_rows(plane, k):
        low = jnp.dot(plane[:, :half], along[k, :half, :half], preferred_element_type=jnp.float32)
        cut = half - RY
        high = jnp.dot(plane[:, cut:], along[k, cut:, half:], preferred_element_type=jnp.float32)
        beyond = pltpu.roll(plane[:, half : half + LANES].astype(jnp.float32), LANES - 1, 1)
        beyond = beyond * brims[k, 0:1, :]
        low = jnp.concatenate([low[:, : half - LANES], low[:, half - LANES :] + beyond], axis=1)
        return low, high

    def mix(now, later, k, number):
        lanes = slice(number * half, (number + 1) * half)
        fraction = (shifts_ref[k] // 16 % 4).astype(jnp.float32) * 0.25
        mixed = now * (1.0 - fraction) + later * fraction
        held[k, :, lanes] = later
        top = mixed.astype(jnp.bfloat16)
        rest = (mixed - top.astype(jnp.float32)).astype(jnp.bfloat16)
        parts[2 * k * length : (2 * k + 1) * length, lanes] = top
        parts[(2 * k + 1) * length : (2 * k + 2) * length, lanes] = rest

    small = [
        pltpu.make_async_copy(source, target, small_sem.at[number])
        for number, (source, target) in enumerate(
            ((offsets_hbm, offsets_ref), (shifts_hbm, shifts_ref), (counts_hbm, counts_ref))
        )
    ]
    for copy in small:
        copy.start()
    for n in range(2):
        fetch(n).start()
    barrier = pltpu.get_barrier_semaphore()
    peers = (
        (has_left, to_left), (has_right, to_right), (has_below, to_below), (has_above, to_above),
        (far_left, to_far_left), (far_right, to_far_right),
    )
    for there, device in peers:
        @pl.when(there)
        def _():
            pl.semaphore_signal(barrier, inc=1, device_id=device, device_id_type=MESH)
    for copy in small:
        copy.wait()
    for n in range(2, RING):
        fetch(n).start()

    starts_x = [offsets_ref[0, k] - column * BX for k in range(slots)]
    starts_y = [offsets_ref[1, k] - row * BY for k in range(slots)]
    active = [jnp.where(k < counts_ref[0, 0], 1.0, 0.0) for k in range(slots)]
    shape = places.shape[1:]
    lane, tile = whole_iota(shape, 1), whole_iota(shape, 0)
    record = jnp.zeros(shape, jnp.float32)
    for k in range(slots):
        values = (starts_x[k].astype(jnp.float32), starts_y[k].astype(jnp.float32), active[k])
        for place, value in enumerate(values):
            record = jnp.where((tile == k) & (lane == place), value, record)
    places[0] = record
    for number in range(1, places.shape[0]):
        there = (has_below, has_above, has_left, has_right)[
            number - 1 if number < 3 else number // 3 + 1
        ]

        @pl.when(jnp.logical_not(there))
        def _():
            places[number] = jnp.zeros(shape, jnp.float32)

    for k in range(slots):
        fraction = (shifts_ref[k] % 4).astype(jnp.float32) * 0.25
        target = whole_iota((1, extent_y), 1) - (starts_y[k] + RY)
        ramp = ramp_at(target, rows)
        here = jnp.where(target == rows - 1, ramp, ramp * (1.0 - fraction))
        after = ramp * fraction
        edge = slice(half - LANES, half)
        brim = jnp.where(target[:, edge] == half - 1, after[:, edge], 0.0)
        brim = jnp.where(whole_iota((1, LANES), 1) == LANES - 1, brim, 0.0)
        brims[k] = jnp.broadcast_to(brim, brims.shape[1:])
        for first, last, lanes in ((0, half, slice(0, half)), (half - RY, rows, slice(half, extent_y))):
            source = whole_iota((last - first, half), 0) + first
            blend = jnp.where(
                source == target[:, lanes], here[:, lanes],
                jnp.where(source == target[:, lanes] + 1, after[:, lanes], 0.0),
            )
            along[k, first:last, lanes] = blend.astype(jnp.bfloat16)
    fetch(0).wait()
    fetch(1).wait()
    for k in range(slots):
        both = planes[k, :2].reshape(2 * length, rows)
        for number, rising in enumerate(along_rows(both, k)):
            mix(rising[:length], rising[length:], k, number)
    fetch(RING).start()
    wide = 2 * slots * length
    number = whole_iota((1, wide), 1)
    part = number // length
    source = number - part * length
    part = part // 2
    fraction = pick(
        part, [(shifts_ref[k] // 4 % 4).astype(jnp.float32) * 0.25 for k in range(slots)]
    )
    weight = pick(part, active)
    ramp = ramp_at(source, length) * weight
    here = jnp.where(source == length - 1, ramp, ramp * (1.0 - fraction))
    after = ramp_at(source - 1, length) * weight * fraction
    target = source + pick(part, [start + RX for start in starts_x])
    cell = whole_iota((extent_x, wide), 0)
    blend = jnp.where(cell == target, here, jnp.where(cell == target - 1, after, 0.0))
    across[...] = blend.astype(jnp.bfloat16)

    def merge(n, part, there):
        @pl.when((n >= 0) & (n < count))
        def _():
            @pl.when(there & (part == 0))
            def _():
                edge_above(n).wait_recv()

            @pl.when(there & (part == 1))
            def _():
                edge_below(n).wait_recv()

            @pl.when(there)
            def _():
                strips[0, part, n] += edges_in[part, n, :RX]
                strips[1, part, n] += edges_in[part, n, RX:]

            for unit in units:
                @pl.when(n == unit[1] + unit[2] - 1)
                def _():
                    send_unit(unit, part)

    lag_near = jnp.where(has_near, LAG_NEAR, 0)
    lag_far = jnp.where(has_far, LAG_FAR, 0)

    def outer(s, left, right):
        edges[0, s, :RX] = left[:, :RY]
        edges[0, s, RX:] = right[:, :RY]
        edges[1, s, :RX] = left[:, RY + BY :]
        edges[1, s, RX:] = right[:, RY + BY :]
        for part in (0, 1):
            strips[0, part, s] = left[:, (part + 1) * RY : (part + 2) * RY]
            strips[1, part, s] = right[:, (part + 1) * RY : (part + 2) * RY]

    def send_edges(s):
        @pl.when(has_below)
        def _():
            edge_below(s).start()

        @pl.when(has_above)
        def _():
            edge_above(s).start()

    def inner(s, centre):
        middles[0, s] = centre[:, :RY]
        middles[1, s] = centre[:, RY + BY :]
        out_ref[s] = centre[:, RY : RY + BY]

    def merges(s):
        merge(s - lag_near, near, has_near)
        merge(s - lag_far, far, has_far)

    def step(s, carry):
        @pl.when(s < count)
        def _():
            @pl.when(s < count - 1)
            def _():
                fetch(s + 1).wait()

            slot = jnp.minimum(s + 1, count - 1) % RING
            for k in range(slots):
                for number, later in enumerate(along_rows(planes[k, slot], k)):
                    mix(held[k, :, number * half : (number + 1) * half], later, k, number)

            @pl.when(s + 1 + RING < count)
            def _():
                fetch(s + 1 + RING).start()

            total = jnp.dot(across[...], parts[...], preferred_element_type=jnp.float32)
            outer(s, total[:RX], total[RX + BX :])
            send_edges(s)
            inner(s, total[RX : RX + BX])

        merges(s)

        @pl.when(s == LAG_PLACE)
        def _():
            @pl.when(has_below)
            def _():
                place_above.wait_recv()

            @pl.when(has_above)
            def _():
                place_below.wait_recv()

            @pl.when(has_right)
            def _():
                place_right.start()

            @pl.when(has_left)
            def _():
                place_left.start()

        return carry

    total = jnp.dot(across[...], parts[...], preferred_element_type=jnp.float32)
    outer(0, total[:RX], total[RX + BX :])
    inner(0, total[RX : RX + BX])
    pl.semaphore_wait(barrier, sum(jnp.where(there, 1, 0) for there, device in peers))
    send_edges(0)
    merges(0)

    @pl.when(has_above)
    def _():
        place_above.start()

    @pl.when(has_below)
    def _():
        place_below.start()

    fetch(1 + RING).start()
    lax.fori_loop(1, count + max(LAG_NEAR, LAG_FAR), step, 0)

    for side, there in ((0, has_below), (1, has_above)):
        @pl.when(jnp.logical_not(there))
        def _():
            def clear(n, carry):
                middles_in[side, n] = jnp.zeros(middles_in.shape[2:], jnp.float32)
                return carry

            lax.fori_loop(0, count, clear, 0)

    for side, there in ((0, has_left), (1, has_right)):
        @pl.when(jnp.logical_not(there))
        def _():
            def clear(n, carry):
                arrived[side, n] = jnp.zeros(arrived.shape[2:], jnp.float32)
                return carry

            lax.fori_loop(0, count, clear, 0)

    @pl.when(has_below)
    def _():
        middle(0, to_below).start()

    @pl.when(has_above)
    def _():
        middle(1, to_above).start()

    for there, copy in ((has_above, place_above), (has_below, place_below)):
        @pl.when(there)
        def _():
            copy.wait_send()

    @pl.when(has_left)
    def _():
        place_right.wait_recv()
        place_left.wait_send()

    @pl.when(has_right)
    def _():
        place_left.wait_recv()
        place_right.wait_send()

    total = jnp.zeros((BX, BY), jnp.float32)
    cell_x = whole_iota((BX, 1), 0).astype(jnp.float32)
    cell_y = whole_iota((1, BY), 1).astype(jnp.float32)
    for number in range(places.shape[0]):
        origin_x = float((0, -BX, BX)[number // 3])
        origin_y = float((0, -BY, BY)[number % 3])
        for k in range(slots):
            start_x = places[number, k : k + 1, 0:1] + origin_x
            start_y = places[number, k : k + 1, 1:2] + origin_y
            weight = places[number, k : k + 1, 2:3]
            total += (ramp_at(cell_x - start_x, length) * weight) * ramp_at(cell_y - start_y, rows)
    scale[...] = 1.0 / jnp.maximum(total, 1.0)

    for unit in turning:
        relay_unit(unit)

    @pl.when(has_below)
    def _():
        whole_edges(0, to_below).wait_send()
        middle(0, to_below).wait_send()
        middle(1, to_above).wait_recv()

    @pl.when(has_above)
    def _():
        whole_edges(1, to_above).wait_send()
        middle(1, to_above).wait_send()
        middle(0, to_below).wait_recv()

    def finish(n, carry):
        for part in (0, 1):
            lanes = slice(part * RY, (part + 1) * RY)
            for side in (0, 1):
                cells = slice(side * RX, (side + 1) * RX)
                total = out_ref[n, cells, lanes] + middles_in[part, n, cells]
                total += arrived[side, n, part]
                out_ref[n, cells, lanes] = total * scale[cells, lanes]
        return carry

    for stage in range(STAGES):
        inside = [unit for unit in units if unit[4] == stage]
        first, last = inside[0][1], inside[-1][1] + inside[-1][2]

        @pl.when(has_left)
        def _():
            whole_stage(0, stage, first, last).wait_recv()

        @pl.when(has_right)
        def _():
            whole_stage(1, stage, first, last).wait_recv()

        lax.fori_loop(first, last, finish, 0)

    @pl.when(has_left)
    def _():
        whole_strips(0, to_left).wait_send()

    @pl.when(has_right)
    def _():
        whole_strips(1, to_right).wait_send()

    for kind in range(TURNS - 1):
        right = even & far_right & (kind * pairs < TURNS * (pairs - 1 - pair))
        left = jnp.logical_not(even) & far_left & (kind * pairs < TURNS * pair)

        @pl.when(right | left)
        def _():
            relayed(kind).wait_send()


def local(grid_x, grid_y, tiles, tile_offsets, tile_shifts, tile_counts):
    slots, count, length, rows = tiles.shape
    extent_x, extent_y = BX + 2 * RX, BY + 2 * RY
    turning = sum(min(unit[3]) < TURNS - 1 for unit in units_of(count))
    vmem = lambda *shape: pltpu.VMEM(shape, jnp.float32)
    sems = lambda *shape: pltpu.SemaphoreType.DMA(shape)
    return pl.pallas_call(
        functools.partial(kernel, grid_x, grid_y),
        in_specs=[
            pl.BlockSpec(memory_space=pltpu.HBM),
            pl.BlockSpec(memory_space=pltpu.HBM),
            pl.BlockSpec(memory_space=pltpu.HBM),
            pl.BlockSpec(memory_space=pltpu.HBM),
        ],
        out_specs=pl.BlockSpec(memory_space=pltpu.VMEM),
        out_shape=pltpu.VMEM((count, BX, BY), jnp.float32),
        scratch_shapes=[
            pltpu.SMEM((2, slots), jnp.int32),
            pltpu.SMEM((slots,), jnp.int32),
            pltpu.SMEM((1, 1), jnp.int32),
            pltpu.VMEM((slots, RING, length, rows), jnp.bfloat16),
            vmem(2, 2, count, RX, RY),
            vmem(2, count, 2, RX, RY),
            vmem(2, count, RX, RY),
            vmem(2, count, 2 * RX, RY),
            vmem(2, count, 2 * RX, RY),
            vmem(2, count, BX, RY),
            vmem(2, count, BX, RY),
            vmem(9, 8 * pl.cdiv(slots, 8), LANES),
            pltpu.VMEM((extent_x, 2 * slots * length), jnp.bfloat16),
            pltpu.VMEM((slots, rows, extent_y), jnp.bfloat16),
            vmem(slots, 8, LANES),
            vmem(slots, length, extent_y),
            pltpu.VMEM((2 * slots * length, extent_y), jnp.bfloat16),
            vmem(BX, BY),
            sems(3), sems(RING),
            sems(2), sems(2, STAGES), sems(TURNS - 1), sems(2, turning),
            sems(2), sems(2, FLIGHT),
            sems(2), sems(2),
            sems(4), sems(4),
        ],
        compiler_params=pltpu.CompilerParams(
            collective_id=0, has_side_effects=True, vmem_limit_bytes=52 * 1024 * 1024,
        ),
        name="merged",
    )(tile_offsets, tile_shifts, tile_counts.reshape(1, 1), tiles)


def solution(mesh):
    placed = (
        P(("gx", "gy"), None, None, None),
        P(None, ("gx", "gy")),
        P(("gx", "gy")),
        P(("gx", "gy")),
    )
    return jax.shard_map(
        functools.partial(local, mesh.shape["gx"], mesh.shape["gy"]),
        mesh=mesh, in_specs=placed, out_specs=P(None, "gx", "gy"), check_vma=False,
    )
```
